256 devices in a mesh: clip: 8 (over x_lo, y), tile: 32 (over x_hi, z, core).
Axes of the slice: x: 4 (x_hi: 2, x_lo: 2; x = x_hi * 2 + x_lo), y: 4, z: 8, core: 2. Of those that a mesh axis runs over, the one named last changes fastest.
Arguments:
- clip_features: bfloat16 [8, 9, 96, 32, 128], P('clip', None, 'tile'), may hold values from -6 to 6
- upstream: bfloat16 [8, 9, 96, 32, 128], P('clip', None, 'tile'), may hold values from -3 to 3
- weight: bfloat16 [27, 128, 128], replicated, may hold values from -0.109375 to 0.109375
- conv_bias: float32 [128], replicated, may hold values from -2 to 2
Outputs:
- grad_weight: float32 [3456, 128], P('tile')
- grad_bias: float32 [128], replicated
- penalty: float32 [], replicated
The draws below stay inside these ranges and needn't reach their ends.
All inputs are finite; a program needn't handle non-finite values.
Results may differ from the reference program's by a relative error of at most 0.002.
Values may be sent and summed in bfloat16 or wider, within the bound.
No kernel may reach another device: no remote copies, remote signals or barrier semaphores. Data moves between devices by JAX's collectives and lax.ppermute only.
A program may use at most 64 MiB of HBM per device.

```python
import jax
import jax.numpy as jnp
from jax import lax

C = 128
TAPS = 27
FRAMES = 9
HEIGHT = 32
CLIPS = 8
WIDTH = 96
CELLS = 221184


def block_scale(key, shape, cuts, smallest, largest):
    level = 1.0
    for axis_at, shards_of in cuts:
        steps = jax.random.uniform(jax.random.fold_in(jax.random.fold_in(key, 6), axis_at), (shards_of,), jnp.float32, smallest / len(cuts), largest / len(cuts))
        level = level * jnp.repeat(jnp.exp(steps), shape[axis_at] // shards_of).reshape((-1,) + (1,) * (len(shape) - 1 - axis_at))
    return level


def bell_draw(rng, dims, deviation, limit, shards=(), dtype=jnp.bfloat16):
    gain = block_scale(rng, dims, shards, -0.22, 0.18) if shards else 1.0
    drawn = jax.random.normal(rng, dims, jnp.float32) * deviation * gain
    return jnp.minimum(jnp.maximum(drawn, -limit), limit).astype(dtype)


def setup_inputs(seed: int = 0) -> dict:
    splits = jax.random.split(jax.random.key(seed), 5)
    clip_features = bell_draw(splits[0], (CLIPS, FRAMES, WIDTH, HEIGHT, C), 1.0, 6.0, ((0, 8), (2, 32)))
    upstream = bell_draw(splits[1], (CLIPS, FRAMES, WIDTH, HEIGHT, C), 0.5, 3.0, ((0, 8), (2, 32)))
    weight = bell_draw(splits[2], (TAPS, C, C), (TAPS * C) ** -0.5, 0.109375)
    conv_bias = bell_draw(splits[3], (C,), 0.5, 2.0, (), jnp.float32)
    return {"clip_features": clip_features, "upstream": upstream, "weight": weight, "conv_bias": conv_bias}


r1_weight = 10.0


def slope_of(value):
    return 0.2 + 0.8 * jax.nn.sigmoid(value)


def bend_of(value):
    sigma = jax.nn.sigmoid(value)
    return 0.8 * sigma * (1.0 - sigma)


def pad_cells(field):
    return jnp.pad(field, ((1, 1), (1, 1), (1, 1), (0, 0)))


def conv_clip(field, weight, flipped):
    frames, columns, row_count, channels = field.shape
    padded = pad_cells(field)
    summed = jnp.zeros((frames * columns * row_count, weight.shape[2]), jnp.float32)
    for tap_f in range(3):
        for tap_w in range(3):
            for tap_h in range(3):
                index = 9 * tap_f + 3 * tap_w + tap_h
                if flipped:
                    piece = padded[2 - tap_f:2 - tap_f + frames, 2 - tap_w:2 - tap_w + columns, 2 - tap_h:2 - tap_h + row_count, :]
                    kernel = weight[index].T
                else:
                    piece = padded[tap_f:tap_f + frames, tap_w:tap_w + columns, tap_h:tap_h + row_count, :]
                    kernel = weight[index]
                summed = summed + jnp.dot(piece.reshape(-1, channels), kernel, preferred_element_type=jnp.float32)
    return summed.reshape(frames, columns, row_count, -1)


def wgrad_clip(field, gradients):
    frames, columns, row_count, channels = field.shape
    padded = pad_cells(field)
    flat_grads = gradients.reshape(-1, gradients.shape[-1])
    partials = []
    for tap_f in range(3):
        for tap_w in range(3):
            for tap_h in range(3):
                piece = padded[tap_f:tap_f + frames, tap_w:tap_w + columns, tap_h:tap_h + row_count, :]
                partials.append(lax.dot_general(piece.reshape(-1, channels), flat_grads, (((0,), (0,)), ((), ())), preferred_element_type=jnp.float32))
    return jnp.concatenate(partials, axis=0)


def reference(clip_features, upstream, weight, conv_bias):
    factor = r1_weight / CELLS

    def per_clip(clip_pair):
        features, upstream_clip = clip_pair
        upstream_f = upstream_clip.astype(jnp.float32)
        hidden = conv_clip(features, weight, False) + conv_bias
        grad_h = (upstream_f * slope_of(hidden)).astype(jnp.bfloat16)
        grad_x = conv_clip(grad_h, weight, True)
        squares = jnp.sum(grad_x * grad_x)
        grad_xb = grad_x.astype(jnp.bfloat16)
        back_conv = conv_clip(grad_xb, weight, False)
        curvature = (back_conv * upstream_f * bend_of(hidden)).astype(jnp.bfloat16)
        weight_terms = wgrad_clip(grad_xb, grad_h) + wgrad_clip(features, curvature)
        bias_terms = jnp.sum(curvature.astype(jnp.float32), axis=(0, 1, 2))
        return weight_terms, bias_terms, squares

    weight_terms, bias_terms, squares = lax.map(per_clip, (clip_features, upstream))
    grad_weight = factor * jnp.sum(weight_terms, axis=0)
    grad_bias = factor * jnp.sum(bias_terms, axis=0)
    penalty = 0.5 * factor * jnp.sum(squares)
    return grad_weight, grad_bias, penalty
```

```python
import jax
import jax.numpy as jnp
from jax import lax
from jax.experimental import pallas as pl
from jax.experimental.pallas import tpu as pltpu
from jax.sharding import PartitionSpec as P

r1_weight = 10.0
F32, BF16 = jnp.float32, jnp.bfloat16
C = 128
ROWS = 32
FR = 9
BLOCK = 112


def shifted_store(src, dst, frame, columns):
    for c in range(3):
        v = src[frame, 0:columns, 7 + c : 39 + c, :]
        dst[frame + 1, 0:columns, :, c * C : (c + 1) * C] = v.astype(BF16)


def zero_edges(src, dst, columns):
    src[:, :, 0:8, :] = jnp.zeros((FR, columns, 8, C), F32)
    src[:, :, 40:48, :] = jnp.zeros((FR, columns, 8, C), F32)
    dst[0] = jnp.zeros((columns, ROWS, 3 * C), BF16)
    dst[FR + 1] = jnp.zeros((columns, ROWS, 3 * C), BF16)


def conv(src, f0, frames, columns, weight):
    pieces = []
    for a in range(3):
        for b in range(3):
            v = src[f0 + a : f0 + a + frames, b : b + columns, :, :]
            pieces.append(v.reshape(frames * columns * ROWS, 3 * C))
    lhs = jnp.concatenate(pieces, axis=1)
    return jnp.dot(lhs, weight[...], preferred_element_type=F32)


def kernel(t_ref, x_ref, xp_ref, xb_ref, u_ref, up_ref, ub_ref, w_ref, wf_ref, bias_ref,
           keep_ref, send_ref, xf, x3, ue, gf, g3, ff, f3, bd, cv, gw):
    t = t_ref[0]
    s = lax.rem(t, 2)
    pcol = 6 - 6 * s
    bcol = 6 * s
    zero_edges(xf, x3, 9)
    zero_edges(gf, g3, 7)
    zero_edges(ff, f3, 5)
    xf[:, 3:6, 8:40, :] = x_ref[0].astype(F32)
    xf[:, pl.ds(pcol, 3), 8:40, :] = xp_ref[0].astype(F32)
    xf[:, pl.ds(bcol, 3), 8:40, :] = xb_ref[0].astype(F32)
    ue[:, 3:6] = u_ref[0]
    ue[:, pl.ds(pcol, 3)] = up_ref[0]
    ue[:, pl.ds(bcol, 3)] = ub_ref[0]
    for f in range(FR):
        shifted_store(xf, x3, f, 9)
    bias = bias_ref[...]
    for f0 in range(0, FR, 3):
        h = conv(x3, f0, 3, 7, w_ref) + bias
        sig = jax.nn.sigmoid(h).reshape(3, 7, ROWS, C)
        u = ue[f0 : f0 + 3, 1:8].astype(F32)
        gf[f0 : f0 + 3, :, 8:40, :] = u * (0.2 + 0.8 * sig)
        so = sig[:, 2:5]
        bd[f0 : f0 + 3] = u[:, 2:5] * (0.8 * so * (1.0 - so))
        for f in range(f0, f0 + 3):
            shifted_store(gf, g3, f, 7)
    left_in = jnp.where(t > 0, 1.0, 0.0)
    right_in = jnp.where(t < 31, 1.0, 0.0)
    squares = jnp.zeros((8, C), F32)
    for f0 in range(0, FR, 3):
        gx = conv(g3, f0, 3, 5, wf_ref).reshape(3, 5, ROWS, C)
        own = gx[:, 1:4]
        squares = squares + jnp.sum((own * own).reshape(36, 8, C), axis=0)
        ff[f0 : f0 + 3, 1:4, 8:40, :] = own
        ff[f0 : f0 + 3, 0:1, 8:40, :] = gx[:, 0:1] * left_in
        ff[f0 : f0 + 3, 4:5, 8:40, :] = gx[:, 4:5] * right_in
        for f in range(f0, f0 + 3):
            shifted_store(ff, f3, f, 5)
    bias_sum = jnp.zeros((8, C), F32)
    for f0 in range(0, FR, 3):
        bc = conv(f3, f0, 3, 3, w_ref).reshape(3, 3, ROWS, C)
        cu = (bc * bd[f0 : f0 + 3]).astype(BF16).astype(F32)
        bias_sum = bias_sum + jnp.sum(cu.reshape(36, 8, C), axis=0)
        cv[f0 : f0 + 3] = cu
    right = jnp.concatenate(
        [gf[:, 2:5, 8:40, :].reshape(FR * 96, C), cv[...].reshape(FR * 96, C)], axis=0
    )
    rt = right.T.astype(BF16)
    for a in range(3):
        cols = []
        for b in range(3):
            cols.append(
                jnp.concatenate(
                    [
                        f3[a : a + FR, b : b + 3].reshape(FR * 96, 3 * C),
                        x3[a : a + FR, 2 + b : 5 + b].reshape(FR * 96, 3 * C),
                    ],
                    axis=0,
                )
            )
        left = jnp.concatenate(cols, axis=1)
        g = jnp.dot(rt, left, preferred_element_type=F32)
        for k in range(9):
            gw[(9 * a + k) * C : (9 * a + k + 1) * C, :] = g[:, k * C : (k + 1) * C].T
    bias_row = jnp.sum(bias_sum, axis=0, keepdims=True)
    sq_row = jnp.sum(squares, axis=0, keepdims=True)
    stats = jnp.concatenate([bias_row, bias_row, sq_row, sq_row], axis=0)
    for core in range(2):

        @pl.when(s == core)
        def _():
            for j in range(32):
                ref = keep_ref if j % 2 == core else send_ref
                ref[j // 2, 0:108, :] = gw[108 * j : 108 * j + 108, :]
                ref[j // 2, 108:112, :] = stats


def compute(t, x, xp, xb, u, up, ub, w, wf, bias):
    vm = pl.BlockSpec(memory_space=pltpu.VMEM)
    return pl.pallas_call(
        kernel,
        in_specs=[pl.BlockSpec(memory_space=pltpu.SMEM)] + [vm] * 9,
        out_specs=[vm, vm],
        out_shape=[jax.ShapeDtypeStruct((16, BLOCK, C), F32)] * 2,
        scratch_shapes=[
            pltpu.VMEM((FR, 9, 48, C), F32),
            pltpu.VMEM((FR + 2, 9, ROWS, 3 * C), BF16),
            pltpu.VMEM((FR, 9, ROWS, C), BF16),
            pltpu.VMEM((FR, 7, 48, C), F32),
            pltpu.VMEM((FR + 2, 7, ROWS, 3 * C), BF16),
            pltpu.VMEM((FR, 5, 48, C), F32),
            pltpu.VMEM((FR + 2, 5, ROWS, 3 * C), BF16),
            pltpu.VMEM((FR, 3, ROWS, C), F32),
            pltpu.VMEM((FR, 3, ROWS, C), F32),
            pltpu.VMEM((27 * C, C), F32),
        ],
        compiler_params=pltpu.CompilerParams(vmem_limit_bytes=48 * 1024 * 1024),
        name="r1_section",
    )(t, x, xp, xb, u, up, ub, w, wf, bias)


def shards(clip_features, upstream, weight, conv_bias):
    tiles = 32
    factor = r1_weight / 221184
    w = weight.reshape(27 * C, C)
    wf = jnp.swapaxes(weight[::-1], 1, 2).reshape(27 * C, C)
    swap = [(i, i ^ 1) for i in range(tiles)]
    pairs = []
    for i in range(1, tiles - 1, 2):
        pairs += [(i, i + 1), (i + 1, i)]
    xb = lax.ppermute(clip_features, "tile", pairs)
    xp = lax.ppermute(clip_features, "tile", swap)
    up = lax.ppermute(upstream, "tile", swap)
    ub = lax.ppermute(upstream, "tile", pairs)
    t = lax.axis_index("tile").astype(jnp.int32).reshape(1)
    keep, send = compute(t, clip_features, xp, xb, upstream, up, ub, w, wf, conv_bias.reshape(1, C))
    both = keep + lax.ppermute(send, "tile", swap)
    row = lax.broadcasted_iota(jnp.int32, (1, BLOCK, 1), 1)
    low = (row == 109) | (row == 111)
    rounded = lax.reduce_precision(both, 8, 7)
    both = jnp.where(low, both - rounded, both).astype(BF16)
    groups = [[2 * i + c for i in range(16)] for c in range(2)]
    got = lax.all_to_all(both, "tile", 0, 0, axis_index_groups=groups, tiled=True)
    mine = jnp.sum(got.astype(F32), axis=0)
    everyone = lax.all_to_all(
        jnp.broadcast_to(mine[None], (8, BLOCK, C)), "clip", 0, 0, tiled=True
    )
    total = jnp.sum(everyone, axis=0)
    grad_bias = factor * (total[108] + total[109])
    penalty = 0.5 * factor * jnp.sum(total[110] + total[111])
    return factor * total[:108], grad_bias, penalty


def solution(mesh):
    in_specs = (P("clip", None, "tile", None, None), P("clip", None, "tile", None, None), P(), P())
    out_specs = (P("tile", None), P(), P())
    return jax.shard_map(shards, mesh=mesh, in_specs=in_specs, out_specs=out_specs, check_vma=False)
```

```python
import jax
import jax.numpy as jnp
from jax import lax
from jax.experimental import pallas as pl
from jax.experimental.pallas import tpu as pltpu
from jax.sharding import PartitionSpec as P

r1_weight = 10.0
factor = r1_weight / 221184
F32, BF16 = jnp.float32, jnp.bfloat16
C = 128
ROWS = 32
FR = 9
TILES = 32
BLOCK = 112


def place(frame):
    return (frame + 1) // 2, (frame + 1) % 2


def spread_rows(src, dst, frames, src_col, dst_col, columns):
    for f in frames:
        p, r = place(f)
        for c in range(3):
            v = src[f, pl.ds(src_col, columns), 7 + c : 39 + c, :]
            dst[p, r, pl.ds(dst_col, columns), :, c * C : (c + 1) * C] = v.astype(BF16)


def zero_rows(src, columns):
    src[:, :, 0:8, :] = jnp.zeros((FR, columns, 8, C), F32)
    src[:, :, 40:48, :] = jnp.zeros((FR, columns, 8, C), F32)


def zero_frames(dst, columns):
    for f in (-1, 9, 10):
        p, r = place(f)
        dst[p, r] = jnp.zeros((columns, ROWS, 3 * C), BF16)


def conv(src, p0, pairs, col, columns, weight):
    pieces = []
    for a in range(4):
        for b in range(3):
            p = p0 + a // 2
            v = src[p : p + pairs, a % 2, pl.ds(col + b, columns), :, :]
            pieces.append(v.reshape(pairs * columns * ROWS, 3 * C))
    lhs = jnp.concatenate(pieces, axis=1)
    out = jnp.dot(lhs, weight[...], preferred_element_type=F32)
    out = out.reshape(pairs, columns, ROWS, 2 * C)
    return [
        (2 * (p0 + i) + r, out[i, :, :, r * C : (r + 1) * C])
        for i in range(pairs)
        for r in range(2)
        if 2 * (p0 + i) + r < FR
    ]


GROUPS = ((0, 3), (3, 2))


def hidden_part(x3, ue, gf, bd, g3, weight, bias, col, columns):
    for p0, pairs in GROUPS:
        for f, out in conv(x3, p0, pairs, col, columns, weight):
            sig = jax.nn.sigmoid(out + bias)
            u = ue[f, pl.ds(col + 1, columns)].astype(F32)
            gf[f, 0:columns, 8:40, :] = u * (0.2 + 0.8 * sig)
            bd[f, pl.ds(col, columns)] = u * (0.8 * sig * (1.0 - sig))
            spread_rows(gf, g3, (f,), 0, col, columns)


def grad_part(g3, ff, f3, weight, col, columns, masks, shares):
    squares = [jnp.zeros((8, C), F32) for _ in range(columns)]
    for p0, pairs in GROUPS:
        for f, gx in conv(g3, p0, pairs, col, columns, weight):
            for q in range(columns):
                v = gx[q]
                if masks[q] is not None:
                    v = v * masks[q]
                ff[f, q, 8:40, :] = v
                squares[q] = squares[q] + jnp.sum((v * v).reshape(4, 8, C), axis=0)
            spread_rows(ff, f3, (f,), 0, col, columns)
    return sum(v * share for v, share in zip(squares, shares))


def gather_kernel(t_ref, x_ref, u_ref, own_ref, edge_ref, sems):
    s = lax.rem(t_ref[0], 2)
    copies = (
        pltpu.make_async_copy(x_ref.at[0], edge_ref.at[:, pl.ds(0, 3)], sems.at[0]),
        pltpu.make_async_copy(u_ref.at[0, :, pl.ds(s, 2)], edge_ref.at[:, pl.ds(3, 2)], sems.at[1]),
        pltpu.make_async_copy(x_ref.at[0], own_ref.at[0], sems.at[2]),
        pltpu.make_async_copy(u_ref.at[0], own_ref.at[1], sems.at[3]),
    )
    for copy in copies:
        copy.start()
    for copy in copies:
        copy.wait()


def near_kernel(t_ref, o_ref, p_ref, w_ref, bias_ref,
                x3, g3, f3, bd, wp, wfp, bias, sq, xf, ue, gf, ff, sems):
    s = lax.rem(t_ref[0], 2)
    pcol = 6 - 6 * s
    copies = (
        pltpu.make_async_copy(w_ref, wp.at[0 : 27 * C, 0:C], sems.at[0]),
        pltpu.make_async_copy(w_ref, wp.at[9 * C : 36 * C, C : 2 * C], sems.at[1]),
        pltpu.make_async_copy(bias_ref, bias, sems.at[2]),
    )
    for copy in copies:
        copy.start()
    for m in (wp, wfp):
        m[27 * C : 36 * C, 0:C] = jnp.zeros((9 * C, C), BF16)
        m[0 : 9 * C, C : 2 * C] = jnp.zeros((9 * C, C), BF16)
    zero_rows(xf, 6)
    zero_rows(gf, 4)
    zero_rows(ff, 2)
    zero_frames(x3, 9)
    zero_frames(g3, 7)
    zero_frames(f3, 5)
    xf[:, 0:3, 8:40, :] = o_ref[0].astype(F32)
    xf[:, 3:6, 8:40, :] = p_ref[0].astype(F32)
    ue[:, 3:6] = o_ref[1]
    ue[:, pl.ds(pcol, 3)] = p_ref[1]
    spread_rows(xf, x3, range(FR), 0, 3, 3)
    spread_rows(xf, x3, range(FR), 3, pcol, 3)
    for copy in copies:
        copy.wait()
    for k in range(27):
        tap = wp[(26 - k) * C : (27 - k) * C, 0:C].astype(F32).T.astype(BF16)
        wfp[k * C : (k + 1) * C, 0:C] = tap
        wfp[(k + 9) * C : (k + 10) * C, C : 2 * C] = tap
    hidden_part(x3, ue, gf, bd, g3, wp, bias[...], 3 - 3 * s, 4)
    odd = s.astype(F32)
    sq[...] = grad_part(g3, ff, f3, wfp, 3 - 3 * s, 2, (None, None), (1.0 - odd, odd))


def far_kernel(t_ref, o_ref, b_ref, wp, wfp, bias_ref, sq_ref,
               x3_in, g3_in, f3_in, bd_in, keep_ref, send_ref, x3, g3, f3, bd,
               xf, ue, gf, ff, cv, gw):
    t = t_ref[0]
    s = lax.rem(t, 2)
    bcol = 6 * s
    zero_rows(xf, 3)
    zero_rows(gf, 3)
    zero_rows(ff, 3)
    xf[:, :, 8:40, :] = b_ref[:, 0:3].astype(F32)
    ue[:, 3:6] = o_ref[1]
    ue[:, pl.ds(1 + 5 * s, 2)] = b_ref[:, 3:5]
    spread_rows(xf, x3, range(FR), 0, bcol, 3)
    hidden_part(x3, ue, gf, bd, g3, wp, bias_ref[...], 4 * s, 3)
    odd = s.astype(F32)
    left_in = jnp.where(t == 0, 0.0, 1.0)
    right_in = jnp.where(t == TILES - 1, 0.0, 1.0)
    squares = sq_ref[...] + grad_part(
        g3, ff, f3, wfp, 2 * s, 3, (left_in, None, right_in), (odd, 1.0, 1.0 - odd)
    )
    bias_sum = jnp.zeros((8, C), F32)
    for p0, pairs in GROUPS:
        for f, bc in conv(f3, p0, pairs, 0, 3, wp):
            cu = (bc * bd[f, 2:5]).astype(BF16).astype(F32)
            bias_sum = bias_sum + jnp.sum(cu.reshape(12, 8, C), axis=0)
            cv[f] = cu
    own = [g3[(*place(f), slice(2, 5), slice(None), slice(C, 2 * C))] for f in range(FR)]
    own = jnp.concatenate([v.astype(F32).reshape(96, C) for v in own], axis=0)
    right = jnp.concatenate([own, cv[...].reshape(FR * 96, C)], axis=0)
    rt = right.T.astype(BF16)
    for a in range(3):
        cols = []
        for b in range(3):
            taps = [f3[(*place(f + a - 1), slice(b, b + 3))] for f in range(FR)]
            taps += [x3[(*place(f + a - 1), slice(2 + b, 5 + b))] for f in range(FR)]
            cols.append(jnp.concatenate([v.reshape(96, 3 * C) for v in taps], axis=0))
        left = jnp.concatenate(cols, axis=1)
        g = jnp.dot(rt, left, preferred_element_type=F32)
        for k in range(9):
            gw[(9 * a + k) * C : (9 * a + k + 1) * C, :] = g[:, k * C : (k + 1) * C].T
    bias_row = jnp.sum(bias_sum, axis=0, keepdims=True)
    sq_row = jnp.sum(squares, axis=0, keepdims=True)
    stats = jnp.concatenate([bias_row, bias_row, sq_row, sq_row], axis=0)
    for core in range(2):

        @pl.when(s == core)
        def _():
            for j in range(TILES):
                ref = keep_ref if j % 2 == core else send_ref
                ref[j // 2, 0:108, :] = gw[108 * j : 108 * j + 108, :]
                ref[j // 2, 108:112, :] = stats


def high_and_low(total):
    high = total.astype(BF16).astype(F32)
    return high, total - high


def middle_kernel(got_ref, out_ref):
    total = jnp.sum(got_ref[...].astype(F32), axis=0)
    bias = high_and_low(total[108:109] + total[109:110])
    squares = high_and_low(total[110:111] + total[111:112])
    full = jnp.concatenate([total[0:108], *bias, *squares], axis=0).astype(BF16)
    for i in range(8):
        out_ref[i] = full


def last_kernel(got_ref, grad_ref, bias_ref, penalty_ref):
    total = jnp.sum(got_ref[...].astype(F32), axis=0)
    grad_ref[...] = factor * total[0:108]
    bias_ref[...] = factor * (total[108:109] + total[109:110])
    square = jnp.sum(total[110:111] + total[111:112], axis=1, keepdims=True)
    penalty_ref[...] = 0.5 * factor * square


VM = pl.BlockSpec(memory_space=pltpu.VMEM)
SM = pl.BlockSpec(memory_space=pltpu.SMEM)
HB = pl.BlockSpec(memory_space=pltpu.HBM)


def params(mib):
    return pltpu.CompilerParams(vmem_limit_bytes=mib * 1024 * 1024)


def shape(dtype, *dims):
    return jax.ShapeDtypeStruct(dims, dtype)


def gather(t, x, u):
    return pl.pallas_call(
        gather_kernel,
        in_specs=[SM, HB, HB],
        out_specs=[VM] * 2,
        out_shape=[shape(BF16, 2, FR, 3, ROWS, C), shape(BF16, FR, 5, ROWS, C)],
        scratch_shapes=[pltpu.SemaphoreType.DMA((4,))],
        compiler_params=params(4),
        name="gather_own",
    )(t, x, u)


def near(t, own, p, w, bias):
    return pl.pallas_call(
        near_kernel,
        in_specs=[SM, VM, VM, HB, HB],
        out_specs=[VM] * 8,
        out_shape=[
            shape(BF16, 6, 2, 9, ROWS, 3 * C),
            shape(BF16, 6, 2, 7, ROWS, 3 * C),
            shape(BF16, 6, 2, 5, ROWS, 3 * C),
            shape(F32, FR, 7, ROWS, C),
            shape(BF16, 36 * C, 2 * C),
            shape(BF16, 36 * C, 2 * C),
            shape(F32, 1, C),
            shape(F32, 8, C),
        ],
        scratch_shapes=[
            pltpu.VMEM((FR, 6, 48, C), F32),
            pltpu.VMEM((FR, 9, ROWS, C), BF16),
            pltpu.VMEM((FR, 4, 48, C), F32),
            pltpu.VMEM((FR, 2, 48, C), F32),
            pltpu.SemaphoreType.DMA((3,)),
        ],
        compiler_params=params(24),
        cost_estimate=pl.CostEstimate(flops=4_000_000_000, bytes_accessed=8_000_000, transcendentals=0),
        name="near_columns",
    )(t, own, p, w, bias)


def far(t, own, b, wp, wfp, bias, sq, x3, g3, f3, bd):
    return pl.pallas_call(
        far_kernel,
        in_specs=[SM] + [VM] * 10,
        out_specs=[VM] * 6,
        out_shape=[shape(F32, 16, BLOCK, C)] * 2
        + [shape(v.dtype, *v.shape) for v in (x3, g3, f3, bd)],
        scratch_shapes=[
            pltpu.VMEM((FR, 3, 48, C), F32),
            pltpu.VMEM((FR, 9, ROWS, C), BF16),
            pltpu.VMEM((FR, 3, 48, C), F32),
            pltpu.VMEM((FR, 3, 48, C), F32),
            pltpu.VMEM((FR, 3, ROWS, C), F32),
            pltpu.VMEM((27 * C, C), F32),
        ],
        input_output_aliases={7: 2, 8: 3, 9: 4, 10: 5},
        compiler_params=params(24),
        cost_estimate=pl.CostEstimate(flops=6_000_000_000, bytes_accessed=8_000_000, transcendentals=0),
        name="far_columns",
    )(t, own, b, wp, wfp, bias, sq, x3, g3, f3, bd)[:2]


def shards(clip_features, upstream, weight, conv_bias):
    w = weight.reshape(27 * C, C)
    bias = conv_bias.reshape(1, C)
    swap = [(i, i ^ 1) for i in range(TILES)]
    pairs = []
    for i in range(1, TILES - 1, 2):
        pairs += [(i, i + 1), (i + 1, i)]
    t = lax.axis_index("tile").astype(jnp.int32).reshape(1)
    in_hbm = lambda v: pltpu.with_memory_space_constraint(v, pltpu.HBM)
    own, edge = gather(t, in_hbm(clip_features), in_hbm(upstream))
    other = lax.ppermute(edge, "tile", pairs)
    partner = lax.ppermute(own, "tile", swap)
    x3, g3, f3, bd, wp, wfp, bias, sq = near(t, own, partner, in_hbm(w), in_hbm(bias))
    keep, send = far(t, own, other, wp, wfp, bias, sq, x3, g3, f3, bd)
    total = keep + lax.ppermute(send, "tile", swap)
    row = lax.broadcasted_iota(jnp.int32, (1, BLOCK, 1), 1)
    low = (row == 109) | (row == 111)
    rounded = lax.reduce_precision(total, 8, 7)
    total = jnp.where(low, total - rounded, total).astype(BF16)
    groups = [[2 * i + c for i in range(16)] for c in range(2)]
    got = lax.all_to_all(total, "tile", 0, 0, axis_index_groups=groups, tiled=True)
    mine = pl.pallas_call(
        middle_kernel,
        in_specs=[VM],
        out_specs=VM,
        out_shape=jax.ShapeDtypeStruct((8, BLOCK, C), BF16),
        compiler_params=params(4),
        name="middle_sum",
    )(got)
    everyone = lax.all_to_all(mine, "clip", 0, 0, tiled=True)
    grad, grad_bias, penalty = pl.pallas_call(
        last_kernel,
        in_specs=[VM],
        out_specs=[VM] * 3,
        out_shape=[
            jax.ShapeDtypeStruct((108, C), F32),
            jax.ShapeDtypeStruct((1, C), F32),
            jax.ShapeDtypeStruct((1, 1), F32),
        ],
        compiler_params=params(4),
        name="last_sum",
    )(everyone)
    return grad, grad_bias.reshape(C), penalty.reshape(())


def solution(mesh):
    in_specs = (P("clip", None, "tile", None, None), P("clip", None, "tile", None, None), P(), P())
    out_specs = (P("tile", None), P(), P())
    return jax.shard_map(shards, mesh=mesh, in_specs=in_specs, out_specs=out_specs, check_vma=False)
```

```python
import jax
import jax.numpy as jnp
from jax import lax
from jax.experimental import pallas as pl
from jax.experimental.pallas import tpu as pltpu
from jax.sharding import PartitionSpec as P

r1_weight = 10.0
factor = r1_weight / 221184
F32, BF16 = jnp.float32, jnp.bfloat16
C = 128
ROWS = 32
FR = 9
TILES = 32
BLOCK = 112


def place(frame):
    return (frame + 1) // 2, (frame + 1) % 2


def spread_rows(src, dst, frames, src_col, dst_col, columns):
    for f in frames:
        p, r = place(f)
        for c in range(3):
            v = src[f, pl.ds(src_col, columns), 7 + c : 39 + c, :]
            dst[p, r, pl.ds(dst_col, columns), :, c * C : (c + 1) * C] = v.astype(BF16)


def zero_rows(src, columns):
    src[:, :, 0:8, :] = jnp.zeros((FR, columns, 8, C), F32)
    src[:, :, 40:48, :] = jnp.zeros((FR, columns, 8, C), F32)


def zero_frames(dst, columns):
    for f in (-1, 9, 10):
        p, r = place(f)
        dst[p, r] = jnp.zeros((columns, ROWS, 3 * C), BF16)


def conv(src, p0, pairs, col, columns, weight):
    pieces = []
    for a in range(4):
        for b in range(3):
            p = p0 + a // 2
            v = src[p : p + pairs, a % 2, pl.ds(col + b, columns), :, :]
            pieces.append(v.reshape(pairs * columns * ROWS, 3 * C))
    lhs = jnp.concatenate(pieces, axis=1)
    out = jnp.dot(lhs, weight[...], preferred_element_type=F32)
    out = out.reshape(pairs, columns, ROWS, 2 * C)
    return [
        (2 * (p0 + i) + r, out[i, :, :, r * C : (r + 1) * C])
        for i in range(pairs)
        for r in range(2)
        if 2 * (p0 + i) + r < FR
    ]


GROUPS = ((0, 2), (2, 2), (4, 1))


def hidden_part(x3, ue, gf, bd, g3, weight, bias, col, columns):
    for p0, pairs in GROUPS:
        for f, out in conv(x3, p0, pairs, col, columns, weight):
            sig = jax.nn.sigmoid(out + bias)
            u = ue[f, pl.ds(col + 1, columns)].astype(F32)
            gf[f, 0:columns, 8:40, :] = u * (0.2 + 0.8 * sig)
            bd[f, pl.ds(col, columns)] = u * (0.8 * sig * (1.0 - sig))
            spread_rows(gf, g3, (f,), 0, col, columns)


def grad_part(g3, ff, f3, weight, col, columns, masks, shares):
    squares = jnp.zeros((8, C), F32)
    for p0, pairs in GROUPS:
        for f, gx in conv(g3, p0, pairs, col, columns, weight):
            for q in range(columns):
                v = gx[q]
                if masks[q] is not None:
                    v = v * masks[q]
                ff[f, q, 8:40, :] = v
                if shares[q]:
                    squares = squares + jnp.sum((v * v).reshape(4, 8, C), axis=0)
            spread_rows(ff, f3, (f,), 0, col, columns)
    return squares


def gather_kernel(t_ref, x_ref, u_ref, own_ref, edge_ref, sems):
    s = lax.rem(t_ref[0], 2)
    copies = (
        pltpu.make_async_copy(x_ref.at[0], edge_ref.at[:, pl.ds(0, 3)], sems.at[0]),
        pltpu.make_async_copy(u_ref.at[0, :, pl.ds(s, 2)], edge_ref.at[:, pl.ds(3, 2)], sems.at[1]),
        pltpu.make_async_copy(x_ref.at[0], own_ref.at[0], sems.at[2]),
        pltpu.make_async_copy(u_ref.at[0], own_ref.at[1], sems.at[3]),
    )
    for copy in copies:
        copy.start()
    for copy in copies:
        copy.wait()


def near_kernel(t_ref, *refs):
    s = lax.rem(t_ref[0], 2)
    for parity in range(2):
        pl.when(s == parity)(lambda: near_body(parity, *refs))


def near_body(s, o_ref, p_ref, w_ref, bias_ref,
              x3, g3, f3, bd, wp, wfp, bias, sq, xf, ue, gf, ff, sems):
    pcol = 6 - 6 * s
    copies = (
        pltpu.make_async_copy(w_ref, wp.at[0 : 27 * C, 0:C], sems.at[0]),
        pltpu.make_async_copy(w_ref, wp.at[9 * C : 36 * C, C : 2 * C], sems.at[1]),
        pltpu.make_async_copy(bias_ref, bias, sems.at[2]),
    )
    for copy in copies:
        copy.start()
    for m in (wp, wfp):
        m[27 * C : 36 * C, 0:C] = jnp.zeros((9 * C, C), BF16)
        m[0 : 9 * C, C : 2 * C] = jnp.zeros((9 * C, C), BF16)
    zero_rows(xf, 6)
    zero_rows(gf, 4)
    zero_rows(ff, 2)
    zero_frames(x3, 9)
    zero_frames(g3, 7)
    zero_frames(f3, 5)
    xf[:, 0:3, 8:40, :] = o_ref[0].astype(F32)
    xf[:, 3:6, 8:40, :] = p_ref[0].astype(F32)
    ue[:, 3:6] = o_ref[1]
    ue[:, pl.ds(pcol, 3)] = p_ref[1]
    spread_rows(xf, x3, range(FR), 0, 3, 3)
    spread_rows(xf, x3, range(FR), 3, pcol, 3)
    for copy in copies:
        copy.wait()
    for k in range(27):
        tap = wp[(26 - k) * C : (27 - k) * C, 0:C].astype(F32).T.astype(BF16)
        wfp[k * C : (k + 1) * C, 0:C] = tap
        wfp[(k + 9) * C : (k + 10) * C, C : 2 * C] = tap
    hidden_part(x3, ue, gf, bd, g3, wp, bias[...], 3 - 3 * s, 4)
    sq[...] = grad_part(g3, ff, f3, wfp, 3 - 3 * s, 2, (None, None), (1 - s, s))


def far_kernel(t_ref, *refs):
    t = t_ref[0]
    s = lax.rem(t, 2)
    for parity in range(2):
        pl.when(s == parity)(lambda: far_body(t, parity, *refs))


def far_body(t, s, o_ref, b_ref, wp, wfp, bias_ref, sq_ref,
             x3_in, g3_in, f3_in, bd_in, keep_ref, send_ref, x3, g3, f3, bd,
             xf, ue, gf, ff, cv, gw):
    bcol = 6 * s
    zero_rows(xf, 3)
    zero_rows(gf, 3)
    zero_rows(ff, 3)
    xf[:, :, 8:40, :] = b_ref[:, 0:3].astype(F32)
    ue[:, 3:6] = o_ref[1]
    ue[:, pl.ds(1 + 5 * s, 2)] = b_ref[:, 3:5]
    spread_rows(xf, x3, range(FR), 0, bcol, 3)
    hidden_part(x3, ue, gf, bd, g3, wp, bias_ref[...], 4 * s, 3)
    left_in = None if s else jnp.where(t == 0, 0.0, 1.0)
    right_in = jnp.where(t == TILES - 1, 0.0, 1.0) if s else None
    squares = sq_ref[...] + grad_part(
        g3, ff, f3, wfp, 2 * s, 3, (left_in, None, right_in), (s, 1, 1 - s)
    )
    bias_sum = jnp.zeros((8, C), F32)
    for p0, pairs in GROUPS:
        for f, bc in conv(f3, p0, pairs, 0, 3, wp):
            cu = (bc * bd[f, 2:5]).astype(BF16).astype(F32)
            bias_sum = bias_sum + jnp.sum(cu.reshape(12, 8, C), axis=0)
            cv[f] = cu
    own = [g3[(*place(f), slice(2, 5), slice(None), slice(C, 2 * C))] for f in range(FR)]
    own = jnp.concatenate([v.astype(F32).reshape(96, C) for v in own], axis=0)
    right = jnp.concatenate([own, cv[...].reshape(FR * 96, C)], axis=0)
    rt = right.T.astype(BF16)
    bias_row = jnp.sum(bias_sum, axis=0, keepdims=True)
    sq_row = jnp.sum(squares, axis=0, keepdims=True)
    stats = jnp.concatenate([bias_row, bias_row, sq_row, sq_row], axis=0)
    keep_ref[:, 108:112, :] = jnp.broadcast_to(stats, (16, 4, C))
    send_ref[:, 108:112, :] = jnp.broadcast_to(stats, (16, 4, C))
    written = 0
    for first in range(0, 9, 2):
        cols = []
        for ab in range(first, min(first + 2, 9)):
            a, b = ab // 3, ab % 3
            taps = [f3[(*place(f + a - 1), slice(b, b + 3))] for f in range(FR)]
            taps += [x3[(*place(f + a - 1), slice(2 + b, 5 + b))] for f in range(FR)]
            cols.append(jnp.concatenate([v.reshape(96, 3 * C) for v in taps], axis=0))
        left = jnp.concatenate(cols, axis=1)
        g = jnp.dot(rt, left, preferred_element_type=F32)
        for k in range(3 * len(cols)):
            row = (3 * first + k) * C
            gw[row : row + C, :] = g[:, k * C : (k + 1) * C].T
        while written < 16 and 216 * (written + 1) <= 3 * C * (first + len(cols)):
            row = 216 * written
            keep_ref[written, 0:108, :] = gw[row + 108 * s : row + 108 * s + 108, :]
            send_ref[written, 0:108, :] = gw[row + 108 - 108 * s : row + 216 - 108 * s, :]
            written += 1


def high_and_low(total):
    high = total.astype(BF16).astype(F32)
    return high, total - high


def middle_kernel(got_ref, out_ref):
    total = jnp.sum(got_ref[...].astype(F32), axis=0)
    bias = high_and_low(total[108:109] + total[109:110])
    squares = high_and_low(total[110:111] + total[111:112])
    full = jnp.concatenate([total[0:108], *bias, *squares], axis=0).astype(BF16)
    for i in range(8):
        out_ref[i] = full


def last_kernel(got_ref, grad_ref, bias_ref, penalty_ref):
    total = jnp.sum(got_ref[...].astype(F32), axis=0)
    grad_ref[...] = factor * total[0:108]
    bias_ref[...] = factor * (total[108:109] + total[109:110])
    square = jnp.sum(total[110:111] + total[111:112], axis=1, keepdims=True)
    penalty_ref[...] = 0.5 * factor * square


VM = pl.BlockSpec(memory_space=pltpu.VMEM)
SM = pl.BlockSpec(memory_space=pltpu.SMEM)
HB = pl.BlockSpec(memory_space=pltpu.HBM)


def params(mib):
    return pltpu.CompilerParams(vmem_limit_bytes=mib * 1024 * 1024)


def shape(dtype, *dims):
    return jax.ShapeDtypeStruct(dims, dtype)


def gather(t, x, u):
    return pl.pallas_call(
        gather_kernel,
        in_specs=[SM, HB, HB],
        out_specs=[VM] * 2,
        out_shape=[shape(BF16, 2, FR, 3, ROWS, C), shape(BF16, FR, 5, ROWS, C)],
        scratch_shapes=[pltpu.SemaphoreType.DMA((4,))],
        compiler_params=params(4),
        name="gather_own",
    )(t, x, u)


def near(t, own, p, w, bias):
    return pl.pallas_call(
        near_kernel,
        in_specs=[SM, VM, VM, HB, HB],
        out_specs=[VM] * 8,
        out_shape=[
            shape(BF16, 6, 2, 9, ROWS, 3 * C),
            shape(BF16, 6, 2, 7, ROWS, 3 * C),
            shape(BF16, 6, 2, 5, ROWS, 3 * C),
            shape(F32, FR, 7, ROWS, C),
            shape(BF16, 36 * C, 2 * C),
            shape(BF16, 36 * C, 2 * C),
            shape(F32, 1, C),
            shape(F32, 8, C),
        ],
        scratch_shapes=[
            pltpu.VMEM((FR, 6, 48, C), F32),
            pltpu.VMEM((FR, 9, ROWS, C), BF16),
            pltpu.VMEM((FR, 4, 48, C), F32),
            pltpu.VMEM((FR, 2, 48, C), F32),
            pltpu.SemaphoreType.DMA((3,)),
        ],
        compiler_params=params(24),
        cost_estimate=pl.CostEstimate(flops=4_000_000_000, bytes_accessed=8_000_000, transcendentals=0),
        name="near_columns",
    )(t, own, p, w, bias)


def far(t, own, b, wp, wfp, bias, sq, x3, g3, f3, bd):
    return pl.pallas_call(
        far_kernel,
        in_specs=[SM] + [VM] * 10,
        out_specs=[VM] * 6,
        out_shape=[shape(F32, 16, BLOCK, C)] * 2
        + [shape(v.dtype, *v.shape) for v in (x3, g3, f3, bd)],
        scratch_shapes=[
            pltpu.VMEM((FR, 3, 48, C), F32),
            pltpu.VMEM((FR, 9, ROWS, C), BF16),
            pltpu.VMEM((FR, 3, 48, C), F32),
            pltpu.VMEM((FR, 3, 48, C), F32),
            pltpu.VMEM((FR, 3, ROWS, C), F32),
            pltpu.VMEM((27 * C, C), F32),
        ],
        input_output_aliases={7: 2, 8: 3, 9: 4, 10: 5},
        compiler_params=params(24),
        cost_estimate=pl.CostEstimate(flops=6_000_000_000, bytes_accessed=8_000_000, transcendentals=0),
        name="far_columns",
    )(t, own, b, wp, wfp, bias, sq, x3, g3, f3, bd)[:2]


def shards(clip_features, upstream, weight, conv_bias):
    w = weight.reshape(27 * C, C)
    bias = conv_bias.reshape(1, C)
    swap = [(i, i ^ 1) for i in range(TILES)]
    pairs = []
    for i in range(1, TILES - 1, 2):
        pairs += [(i, i + 1), (i + 1, i)]
    t = lax.axis_index("tile").astype(jnp.int32).reshape(1)
    in_hbm = lambda v: pltpu.with_memory_space_constraint(v, pltpu.HBM)
    own, edge = gather(t, in_hbm(clip_features), in_hbm(upstream))
    other = lax.ppermute(edge, "tile", pairs)
    partner = lax.ppermute(own, "tile", swap)
    x3, g3, f3, bd, wp, wfp, bias, sq = near(t, own, partner, in_hbm(w), in_hbm(bias))
    keep, send = far(t, own, other, wp, wfp, bias, sq, x3, g3, f3, bd)
    total = keep + lax.ppermute(send, "tile", swap)
    row = lax.broadcasted_iota(jnp.int32, (1, BLOCK, 1), 1)
    low = (row == 109) | (row == 111)
    rounded = lax.reduce_precision(total, 8, 7)
    total = jnp.where(low, total - rounded, total).astype(BF16)
    groups = [[2 * i + c for i in range(16)] for c in range(2)]
    got = lax.all_to_all(total, "tile", 0, 0, axis_index_groups=groups, tiled=True)
    mine = pl.pallas_call(
        middle_kernel,
        in_specs=[VM],
        out_specs=VM,
        out_shape=jax.ShapeDtypeStruct((8, BLOCK, C), BF16),
        compiler_params=params(4),
        name="middle_sum",
    )(got)
    everyone = lax.all_to_all(mine, "clip", 0, 0, tiled=True)
    grad, grad_bias, penalty = pl.pallas_call(
        last_kernel,
        in_specs=[VM],
        out_specs=[VM] * 3,
        out_shape=[
            jax.ShapeDtypeStruct((108, C), F32),
            jax.ShapeDtypeStruct((1, C), F32),
            jax.ShapeDtypeStruct((1, 1), F32),
        ],
        compiler_params=params(4),
        name="last_sum",
    )(everyone)
    return grad, grad_bias.reshape(C), penalty.reshape(())


def solution(mesh):
    in_specs = (P("clip", None, "tile", None, None), P("clip", None, "tile", None, None), P(), P())
    out_specs = (P("tile", None), P(), P())
    return jax.shard_map(shards, mesh=mesh, in_specs=in_specs, out_specs=out_specs, check_vma=False)
```

```python
import jax
import jax.numpy as jnp
from jax import lax
from jax.experimental import pallas as pl
from jax.experimental.pallas import tpu as pltpu
from jax.sharding import PartitionSpec as P

r1_weight = 10.0
factor = r1_weight / 221184
F32, BF16 = jnp.float32, jnp.bfloat16
C = 128
ROWS = 32
FR = 9
TILES = 32
BLOCK = 112


def place(frame):
    return (frame + 1) // 2, (frame + 1) % 2


def spread_rows(src, dst, frames, src_col, dst_col, columns):
    for f in frames:
        p, r = place(f)
        for c in range(3):
            v = src[f, pl.ds(src_col, columns), 7 + c : 39 + c, :]
            dst[p, r, pl.ds(dst_col, columns), :, c * C : (c + 1) * C] = v.astype(BF16)


def zero_rows(src, columns):
    src[:, :, 0:8, :] = jnp.zeros((FR, columns, 8, C), F32)
    src[:, :, 40:48, :] = jnp.zeros((FR, columns, 8, C), F32)


def zero_frames(dst, columns):
    for f in (-1, 9, 10):
        p, r = place(f)
        dst[p, r] = jnp.zeros((columns, ROWS, 3 * C), BF16)


def conv(src, p0, pairs, col, columns, weight):
    pieces = []
    for a in range(4):
        for b in range(3):
            p = p0 + a // 2
            v = src[p : p + pairs, a % 2, pl.ds(col + b, columns), :, :]
            pieces.append(v.reshape(pairs * columns * ROWS, 3 * C))
    lhs = jnp.concatenate(pieces, axis=1)
    out = jnp.dot(lhs, weight[...], preferred_element_type=F32)
    out = out.reshape(pairs, columns, ROWS, 2 * C)
    return [
        (2 * (p0 + i) + r, out[i, :, :, r * C : (r + 1) * C])
        for i in range(pairs)
        for r in range(2)
        if 2 * (p0 + i) + r < FR
    ]


GROUPS = ((0, 2), (2, 2), (4, 1))


def hidden_part(x3, ue, gf, bd, g3, weight, bias, col, columns):
    for p0, pairs in GROUPS:
        for f, out in conv(x3, p0, pairs, col, columns, weight):
            sig = jax.nn.sigmoid(out + bias)
            u = ue[f, pl.ds(col + 1, columns)].astype(F32)
            gf[f, 0:columns, 8:40, :] = u * (0.2 + 0.8 * sig)
            bd[f, pl.ds(col, columns)] = u * (0.8 * sig * (1.0 - sig))
            spread_rows(gf, g3, (f,), 0, col, columns)


def grad_part(g3, ff, f3, weight, col, columns, masks, shares):
    squares = jnp.zeros((8, C), F32)
    for p0, pairs in GROUPS:
        for f, gx in conv(g3, p0, pairs, col, columns, weight):
            for q in range(columns):
                v = gx[q]
                if masks[q] is not None:
                    v = v * masks[q]
                ff[f, q, 8:40, :] = v
                if shares[q]:
                    squares = squares + jnp.sum((v * v).reshape(4, 8, C), axis=0)
            spread_rows(ff, f3, (f,), 0, col, columns)
    return squares


def gather_kernel(t_ref, x_ref, u_ref, own_ref, edge_ref, sems):
    s = lax.rem(t_ref[0], 2)
    copies = (
        pltpu.make_async_copy(x_ref.at[0], edge_ref.at[:, pl.ds(0, 3)], sems.at[0]),
        pltpu.make_async_copy(u_ref.at[0, :, pl.ds(s, 2)], edge_ref.at[:, pl.ds(3, 2)], sems.at[1]),
        pltpu.make_async_copy(x_ref.at[0], own_ref.at[0], sems.at[2]),
        pltpu.make_async_copy(u_ref.at[0], own_ref.at[1], sems.at[3]),
    )
    for copy in copies:
        copy.start()
    for copy in copies:
        copy.wait()


def near_kernel(t_ref, *refs):
    s = lax.rem(t_ref[0], 2)
    for parity in range(2):
        pl.when(s == parity)(lambda: near_body(parity, *refs))


def near_body(s, o_ref, p_ref, w_ref, bias_ref,
              x3, g3, f3, bd, wp, wfp, bias, sq, xf, ue, gf, ff, sems):
    pcol = 6 - 6 * s
    copies = (
        pltpu.make_async_copy(w_ref, wp.at[0 : 27 * C, 0:C], sems.at[0]),
        pltpu.make_async_copy(w_ref, wp.at[9 * C : 36 * C, C : 2 * C], sems.at[1]),
        pltpu.make_async_copy(bias_ref, bias, sems.at[2]),
    )
    for copy in copies:
        copy.start()
    for m in (wp, wfp):
        m[27 * C : 36 * C, 0:C] = jnp.zeros((9 * C, C), BF16)
        m[0 : 9 * C, C : 2 * C] = jnp.zeros((9 * C, C), BF16)
    zero_rows(xf, 6)
    zero_rows(gf, 4)
    zero_rows(ff, 2)
    zero_frames(x3, 9)
    zero_frames(g3, 7)
    zero_frames(f3, 5)
    xf[:, 0:3, 8:40, :] = o_ref[0].astype(F32)
    xf[:, 3:6, 8:40, :] = p_ref[0].astype(F32)
    ue[:, 3:6] = o_ref[1]
    ue[:, pl.ds(pcol, 3)] = p_ref[1]
    spread_rows(xf, x3, range(FR), 0, 3, 3)
    spread_rows(xf, x3, range(FR), 3, pcol, 3)
    for copy in copies:
        copy.wait()
    for k in range(27):
        tap = wp[(26 - k) * C : (27 - k) * C, 0:C].astype(F32).T.astype(BF16)
        wfp[k * C : (k + 1) * C, 0:C] = tap
        wfp[(k + 9) * C : (k + 10) * C, C : 2 * C] = tap
    hidden_part(x3, ue, gf, bd, g3, wp, bias[...], 3 - 3 * s, 4)
    sq[...] = grad_part(g3, ff, f3, wfp, 3 - 3 * s, 2, (None, None), (1 - s, s))


def far_kernel(t_ref, *refs):
    t = t_ref[0]
    s = lax.rem(t, 2)
    for parity in range(2):
        pl.when(s == parity)(lambda: far_body(t, parity, *refs))


def far_body(t, s, o_ref, b_ref, wp, wfp, bias_ref, sq_ref,
             x3_in, g3_in, f3_in, bd_in, keep_ref, send_ref, x3, g3, f3, bd,
             xf, ue, gf, ff, cv, gw):
    bcol = 6 * s
    zero_rows(xf, 3)
    zero_rows(gf, 3)
    zero_rows(ff, 3)
    xf[:, :, 8:40, :] = b_ref[:, 0:3].astype(F32)
    ue[:, 3:6] = o_ref[1]
    ue[:, pl.ds(1 + 5 * s, 2)] = b_ref[:, 3:5]
    spread_rows(xf, x3, range(FR), 0, bcol, 3)
    hidden_part(x3, ue, gf, bd, g3, wp, bias_ref[...], 4 * s, 3)
    left_in = None if s else jnp.where(t == 0, 0.0, 1.0)
    right_in = jnp.where(t == TILES - 1, 0.0, 1.0) if s else None
    squares = sq_ref[...] + grad_part(
        g3, ff, f3, wfp, 2 * s, 3, (left_in, None, right_in), (s, 1, 1 - s)
    )
    bias_sum = jnp.zeros((8, C), F32)
    for p0, pairs in GROUPS:
        for f, bc in conv(f3, p0, pairs, 0, 3, wp):
            cu = (bc * bd[f, 2:5]).astype(BF16).astype(F32)
            bias_sum = bias_sum + jnp.sum(cu.reshape(12, 8, C), axis=0)
            cv[f] = cu
    own = [g3[(*place(f), slice(2, 5), slice(None), slice(C, 2 * C))] for f in range(FR)]
    own = jnp.concatenate([v.astype(F32).reshape(96, C) for v in own], axis=0)
    right = jnp.concatenate([own, cv[...].reshape(FR * 96, C)], axis=0)
    rt = right.T.astype(BF16)
    bias_row = jnp.sum(bias_sum, axis=0, keepdims=True)
    sq_row = jnp.sum(squares, axis=0, keepdims=True)
    stats = jnp.concatenate([bias_row, bias_row, sq_row, sq_row], axis=0)
    keep_ref[:, 108:112, :] = jnp.broadcast_to(stats, (16, 4, C))
    send_ref[:, 108:112, :] = jnp.broadcast_to(stats, (16, 4, C))
    written = 0
    for first in range(0, 9, 2):
        cols = []
        for ab in range(first, min(first + 2, 9)):
            a, b = ab // 3, ab % 3
            taps = [f3[(*place(f + a - 1), slice(b, b + 3))] for f in range(FR)]
            taps += [x3[(*place(f + a - 1), slice(2 + b, 5 + b))] for f in range(FR)]
            cols.append(jnp.concatenate([v.reshape(96, 3 * C) for v in taps], axis=0))
        left = jnp.concatenate(cols, axis=1)
        g = jnp.dot(rt, left, preferred_element_type=F32)
        for k in range(3 * len(cols)):
            row = (3 * first + k) * C
            gw[row : row + C, :] = g[:, k * C : (k + 1) * C].T
        while written < 16 and 216 * (written + 1) <= 3 * C * (first + len(cols)):
            row = 216 * written
            keep_ref[written, 0:108, :] = gw[row + 108 * s : row + 108 * s + 108, :]
            send_ref[written, 0:108, :] = gw[row + 108 - 108 * s : row + 216 - 108 * s, :]
            written += 1


def high_and_low(total):
    high = total.astype(BF16).astype(F32)
    return high, total - high


def middle_kernel(got_ref, out_ref):
    total = jnp.sum(got_ref[...].astype(F32), axis=0)
    bias = high_and_low(total[108:109] + total[109:110])
    squares = high_and_low(total[110:111] + total[111:112])
    full = jnp.concatenate([total[0:108], *bias, *squares], axis=0).astype(BF16)
    for i in range(8):
        out_ref[i] = full


def last_kernel(got_ref, grad_ref, bias_ref, penalty_ref):
    total = jnp.sum(got_ref[...].astype(F32), axis=0)
    grad_ref[...] = factor * total[0:108]
    bias_ref[...] = factor * (total[108:109] + total[109:110])
    square = jnp.sum(total[110:111] + total[111:112], axis=1, keepdims=True)
    penalty_ref[...] = 0.5 * factor * square


VM = pl.BlockSpec(memory_space=pltpu.VMEM)
SM = pl.BlockSpec(memory_space=pltpu.SMEM)
HB = pl.BlockSpec(memory_space=pltpu.HBM)


def params(mib):
    return pltpu.CompilerParams(vmem_limit_bytes=mib * 1024 * 1024)


def shape(dtype, *dims):
    return jax.ShapeDtypeStruct(dims, dtype)


def gather(t, x, u):
    return pl.pallas_call(
        gather_kernel,
        in_specs=[SM, HB, HB],
        out_specs=[VM] * 2,
        out_shape=[shape(BF16, 2, FR, 3, ROWS, C), shape(BF16, FR, 5, ROWS, C)],
        scratch_shapes=[pltpu.SemaphoreType.DMA((4,))],
        compiler_params=params(4),
        name="gather_own",
    )(t, x, u)


def near(t, own, p, w, bias):
    return pl.pallas_call(
        near_kernel,
        in_specs=[SM, VM, VM, HB, HB],
        out_specs=[VM] * 8,
        out_shape=[
            shape(BF16, 6, 2, 9, ROWS, 3 * C),
            shape(BF16, 6, 2, 7, ROWS, 3 * C),
            shape(BF16, 6, 2, 5, ROWS, 3 * C),
            shape(F32, FR, 7, ROWS, C),
            shape(BF16, 36 * C, 2 * C),
            shape(BF16, 36 * C, 2 * C),
            shape(F32, 1, C),
            shape(F32, 8, C),
        ],
        scratch_shapes=[
            pltpu.VMEM((FR, 6, 48, C), F32),
            pltpu.VMEM((FR, 9, ROWS, C), BF16),
            pltpu.VMEM((FR, 4, 48, C), F32),
            pltpu.VMEM((FR, 2, 48, C), F32),
            pltpu.SemaphoreType.DMA((3,)),
        ],
        compiler_params=params(24),
        cost_estimate=pl.CostEstimate(flops=4_000_000_000, bytes_accessed=8_000_000, transcendentals=0),
        name="near_columns",
    )(t, own, p, w, bias)


def far(t, own, b, wp, wfp, bias, sq, x3, g3, f3, bd):
    return pl.pallas_call(
        far_kernel,
        in_specs=[SM] + [VM] * 10,
        out_specs=[VM] * 6,
        out_shape=[shape(F32, 16, BLOCK, C)] * 2
        + [shape(v.dtype, *v.shape) for v in (x3, g3, f3, bd)],
        scratch_shapes=[
            pltpu.VMEM((FR, 3, 48, C), F32),
            pltpu.VMEM((FR, 9, ROWS, C), BF16),
            pltpu.VMEM((FR, 3, 48, C), F32),
            pltpu.VMEM((FR, 3, 48, C), F32),
            pltpu.VMEM((FR, 3, ROWS, C), F32),
            pltpu.VMEM((27 * C + 8, C), F32),
        ],
        input_output_aliases={7: 2, 8: 3, 9: 4, 10: 5},
        compiler_params=params(24),
        cost_estimate=pl.CostEstimate(flops=6_000_000_000, bytes_accessed=8_000_000, transcendentals=0),
        name="far_columns",
    )(t, own, b, wp, wfp, bias, sq, x3, g3, f3, bd)[:2]


def shards(clip_features, upstream, weight, conv_bias):
    w = weight.reshape(27 * C, C)
    bias = conv_bias.reshape(1, C)
    swap = [(i, i ^ 1) for i in range(TILES)]
    pairs = []
    for i in range(1, TILES - 1, 2):
        pairs += [(i, i + 1), (i + 1, i)]
    t = lax.axis_index("tile").astype(jnp.int32).reshape(1)
    in_hbm = lambda v: pltpu.with_memory_space_constraint(v, pltpu.HBM)
    own, edge = gather(t, in_hbm(clip_features), in_hbm(upstream))
    other = lax.ppermute(edge, "tile", pairs)
    partner = lax.ppermute(own, "tile", swap)
    x3, g3, f3, bd, wp, wfp, bias, sq = near(t, own, partner, in_hbm(w), in_hbm(bias))
    keep, send = far(t, own, other, wp, wfp, bias, sq, x3, g3, f3, bd)
    total = keep + lax.ppermute(send, "tile", swap)
    row = lax.broadcasted_iota(jnp.int32, (1, BLOCK, 1), 1)
    low = (row == 109) | (row == 111)
    rounded = lax.reduce_precision(total, 8, 7)
    total = jnp.where(low, total - rounded, total).astype(BF16)
    groups = [[2 * i + c for i in range(16)] for c in range(2)]
    got = lax.all_to_all(total, "tile", 0, 0, axis_index_groups=groups, tiled=True)
    mine = pl.pallas_call(
        middle_kernel,
        in_specs=[VM],
        out_specs=VM,
        out_shape=jax.ShapeDtypeStruct((8, BLOCK, C), BF16),
        compiler_params=params(4),
        name="middle_sum",
    )(got)
    everyone = lax.all_to_all(mine, "clip", 0, 0, tiled=True)
    grad, grad_bias, penalty = pl.pallas_call(
        last_kernel,
        in_specs=[VM],
        out_specs=[VM] * 3,
        out_shape=[
            jax.ShapeDtypeStruct((108, C), F32),
            jax.ShapeDtypeStruct((1, C), F32),
            jax.ShapeDtypeStruct((1, 1), F32),
        ],
        compiler_params=params(4),
        name="last_sum",
    )(everyone)
    return grad, grad_bias.reshape(C), penalty.reshape(())


def solution(mesh):
    in_specs = (P("clip", None, "tile", None, None), P("clip", None, "tile", None, None), P(), P())
    out_specs = (P("tile", None), P(), P())
    return jax.shard_map(shards, mesh=mesh, in_specs=in_specs, out_specs=out_specs, check_vma=False)
```

```python
import jax
import jax.numpy as jnp
from jax import lax
from jax.experimental import pallas as pl
from jax.experimental.pallas import tpu as pltpu
from jax.sharding import PartitionSpec as P

r1_weight = 10.0
factor = r1_weight / 221184
F32, BF16 = jnp.float32, jnp.bfloat16
C = 128
ROWS = 32
FR = 9
TILES = 32
BLOCK = 112


def place(frame):
    return (frame + 1) // 2, (frame + 1) % 2


def spread_rows(src, dst, frames, src_col, dst_col, columns):
    for f in frames:
        p, r = place(f)
        for c in range(3):
            v = src[f, pl.ds(src_col, columns), 7 + c : 39 + c, :]
            dst[p, r, pl.ds(dst_col, columns), :, c * C : (c + 1) * C] = v.astype(BF16)


def zero_rows(src, columns):
    src[:, :, 0:8, :] = jnp.zeros((FR, columns, 8, C), F32)
    src[:, :, 40:48, :] = jnp.zeros((FR, columns, 8, C), F32)


def zero_frames(dst, columns):
    for f in (-1, 9, 10):
        p, r = place(f)
        dst[p, r] = jnp.zeros((columns, ROWS, 3 * C), BF16)


def conv(src, p0, pairs, col, columns, weight):
    pieces = []
    for a in range(4):
        for b in range(3):
            p = p0 + a // 2
            v = src[p : p + pairs, a % 2, pl.ds(col + b, columns), :, :]
            pieces.append(v.reshape(pairs * columns * ROWS, 3 * C))
    lhs = jnp.concatenate(pieces, axis=1)
    out = jnp.dot(lhs, weight[...], preferred_element_type=F32)
    out = out.reshape(pairs, columns, ROWS, 2 * C)
    return [
        (2 * (p0 + i) + r, out[i, :, :, r * C : (r + 1) * C])
        for i in range(pairs)
        for r in range(2)
        if 2 * (p0 + i) + r < FR
    ]


GROUPS = ((0, 2), (2, 2), (4, 1))


def hidden_part(x3, ue, gf, bd, g3, weight, bias, col, columns):
    for p0, pairs in GROUPS:
        for f, out in conv(x3, p0, pairs, col, columns, weight):
            sig = jax.nn.sigmoid(out + bias)
            u = ue[f, pl.ds(col + 1, columns)].astype(F32)
            gf[f, 0:columns, 8:40, :] = u * (0.2 + 0.8 * sig)
            bd[f, pl.ds(col, columns)] = u * (0.8 * sig * (1.0 - sig))
            spread_rows(gf, g3, (f,), 0, col, columns)


def grad_part(g3, ff, f3, weight, col, columns, masks, shares):
    squares = jnp.zeros((8, C), F32)
    for p0, pairs in GROUPS:
        for f, gx in conv(g3, p0, pairs, col, columns, weight):
            for q in range(columns):
                v = gx[q]
                if masks[q] is not None:
                    v = v * masks[q]
                ff[f, q, 8:40, :] = v
                if shares[q]:
                    squares = squares + jnp.sum((v * v).reshape(4, 8, C), axis=0)
            spread_rows(ff, f3, (f,), 0, col, columns)
    return squares


def gather_kernel(t_ref, x_ref, u_ref, own_ref, edge_ref, sems):
    s = lax.rem(t_ref[0], 2)
    copies = (
        pltpu.make_async_copy(x_ref.at[0], edge_ref.at[:, pl.ds(0, 3)], sems.at[0]),
        pltpu.make_async_copy(u_ref.at[0, :, pl.ds(s, 2)], edge_ref.at[:, pl.ds(3, 2)], sems.at[1]),
        pltpu.make_async_copy(x_ref.at[0], own_ref.at[0], sems.at[2]),
        pltpu.make_async_copy(u_ref.at[0], own_ref.at[1], sems.at[3]),
    )
    for copy in copies:
        copy.start()
    for copy in copies:
        copy.wait()


def own_kernel(o_ref, w_ref, bias_ref, x3, g3, f3, wp, wfp, bias, xf, sems):
    copies = (
        pltpu.make_async_copy(w_ref, wp.at[0 : 27 * C, 0:C], sems.at[0]),
        pltpu.make_async_copy(w_ref, wp.at[9 * C : 36 * C, C : 2 * C], sems.at[1]),
        pltpu.make_async_copy(bias_ref, bias, sems.at[2]),
    )
    for copy in copies:
        copy.start()
    for m in (wp, wfp):
        m[27 * C : 36 * C, 0:C] = jnp.zeros((9 * C, C), BF16)
        m[0 : 9 * C, C : 2 * C] = jnp.zeros((9 * C, C), BF16)
    zero_rows(xf, 3)
    zero_frames(x3, 9)
    zero_frames(g3, 7)
    zero_frames(f3, 5)
    xf[:, :, 8:40, :] = o_ref[0].astype(F32)
    spread_rows(xf, x3, range(FR), 0, 3, 3)
    for copy in copies:
        copy.wait()
    for k in range(27):
        tap = wp[(26 - k) * C : (27 - k) * C, 0:C].astype(F32).T.astype(BF16)
        wfp[k * C : (k + 1) * C, 0:C] = tap
        wfp[(k + 9) * C : (k + 10) * C, C : 2 * C] = tap


def near_kernel(t_ref, *refs):
    s = lax.rem(t_ref[0], 2)
    for parity in range(2):
        pl.when(s == parity)(lambda: near_body(parity, *refs))


def near_body(s, o_ref, p_ref, wp, wfp, bias, x3_in, g3_in, f3_in,
              x3, g3, f3, bd, sq, xf, ue, gf, ff):
    pcol = 6 - 6 * s
    zero_rows(xf, 3)
    zero_rows(gf, 4)
    zero_rows(ff, 2)
    xf[:, :, 8:40, :] = p_ref[0].astype(F32)
    ue[:, 3:6] = o_ref[1]
    ue[:, pl.ds(pcol, 3)] = p_ref[1]
    spread_rows(xf, x3, range(FR), 0, pcol, 3)
    hidden_part(x3, ue, gf, bd, g3, wp, bias[...], 3 - 3 * s, 4)
    sq[...] = grad_part(g3, ff, f3, wfp, 3 - 3 * s, 2, (None, None), (1 - s, s))


def far_kernel(t_ref, *refs):
    t = t_ref[0]
    s = lax.rem(t, 2)
    for parity in range(2):
        pl.when(s == parity)(lambda: far_body(t, parity, *refs))


def far_body(t, s, o_ref, b_ref, wp, wfp, bias_ref, sq_ref,
             x3_in, g3_in, f3_in, bd_in, keep_ref, send_ref, x3, g3, f3, bd,
             xf, ue, gf, ff, cv, gw):
    bcol = 6 * s
    zero_rows(xf, 3)
    zero_rows(gf, 3)
    zero_rows(ff, 3)
    xf[:, :, 8:40, :] = b_ref[:, 0:3].astype(F32)
    ue[:, 3:6] = o_ref[1]
    ue[:, pl.ds(1 + 5 * s, 2)] = b_ref[:, 3:5]
    spread_rows(xf, x3, range(FR), 0, bcol, 3)
    hidden_part(x3, ue, gf, bd, g3, wp, bias_ref[...], 4 * s, 3)
    left_in = None if s else jnp.where(t == 0, 0.0, 1.0)
    right_in = jnp.where(t == TILES - 1, 0.0, 1.0) if s else None
    squares = sq_ref[...] + grad_part(
        g3, ff, f3, wfp, 2 * s, 3, (left_in, None, right_in), (s, 1, 1 - s)
    )
    bias_sum = jnp.zeros((8, C), F32)
    for p0, pairs in GROUPS:
        for f, bc in conv(f3, p0, pairs, 0, 3, wp):
            cu = (bc * bd[f, 2:5]).astype(BF16).astype(F32)
            bias_sum = bias_sum + jnp.sum(cu.reshape(12, 8, C), axis=0)
            cv[f] = cu
    own = [g3[(*place(f), slice(2, 5), slice(None), slice(C, 2 * C))] for f in range(FR)]
    own = jnp.concatenate([v.astype(F32).reshape(96, C) for v in own], axis=0)
    right = jnp.concatenate([own, cv[...].reshape(FR * 96, C)], axis=0)
    rt = right.T.astype(BF16)
    bias_row = jnp.sum(bias_sum, axis=0, keepdims=True)
    sq_row = jnp.sum(squares, axis=0, keepdims=True)
    stats = jnp.concatenate([bias_row, bias_row, sq_row, sq_row], axis=0)
    keep_ref[:, 108:112, :] = jnp.broadcast_to(stats, (16, 4, C))
    send_ref[:, 108:112, :] = jnp.broadcast_to(stats, (16, 4, C))
    written = 0
    for first in range(0, 9, 2):
        cols = []
        for ab in range(first, min(first + 2, 9)):
            a, b = ab // 3, ab % 3
            taps = [f3[(*place(f + a - 1), slice(b, b + 3))] for f in range(FR)]
            taps += [x3[(*place(f + a - 1), slice(2 + b, 5 + b))] for f in range(FR)]
            cols.append(jnp.concatenate([v.reshape(96, 3 * C) for v in taps], axis=0))
        left = jnp.concatenate(cols, axis=1)
        g = jnp.dot(rt, left, preferred_element_type=F32)
        for k in range(3 * len(cols)):
            row = (3 * first + k) * C
            gw[row : row + C, :] = g[:, k * C : (k + 1) * C].T
        while written < 16 and 216 * (written + 1) <= 3 * C * (first + len(cols)):
            row = 216 * written
            keep_ref[written, 0:108, :] = gw[row + 108 * s : row + 108 * s + 108, :]
            send_ref[written, 0:108, :] = gw[row + 108 - 108 * s : row + 216 - 108 * s, :]
            written += 1


def high_and_low(total):
    high = total.astype(BF16).astype(F32)
    return high, total - high


def middle_kernel(got_ref, out_ref):
    total = jnp.sum(got_ref[...].astype(F32), axis=0)
    bias = high_and_low(total[108:109] + total[109:110])
    squares = high_and_low(total[110:111] + total[111:112])
    full = jnp.concatenate([total[0:108], *bias, *squares], axis=0).astype(BF16)
    for i in range(8):
        out_ref[i] = full


def last_kernel(got_ref, grad_ref, bias_ref, penalty_ref):
    total = jnp.sum(got_ref[...].astype(F32), axis=0)
    grad_ref[...] = factor * total[0:108]
    bias_ref[...] = factor * (total[108:109] + total[109:110])
    square = jnp.sum(total[110:111] + total[111:112], axis=1, keepdims=True)
    penalty_ref[...] = 0.5 * factor * square


VM = pl.BlockSpec(memory_space=pltpu.VMEM)
SM = pl.BlockSpec(memory_space=pltpu.SMEM)
HB = pl.BlockSpec(memory_space=pltpu.HBM)


def params(mib):
    return pltpu.CompilerParams(vmem_limit_bytes=mib * 1024 * 1024)


def shape(dtype, *dims):
    return jax.ShapeDtypeStruct(dims, dtype)


def gather(t, x, u):
    return pl.pallas_call(
        gather_kernel,
        in_specs=[SM, HB, HB],
        out_specs=[VM] * 2,
        out_shape=[shape(BF16, 2, FR, 3, ROWS, C), shape(BF16, FR, 5, ROWS, C)],
        scratch_shapes=[pltpu.SemaphoreType.DMA((4,))],
        compiler_params=params(4),
        name="gather_own",
    )(t, x, u)


def prepare(own, w, bias):
    return pl.pallas_call(
        own_kernel,
        in_specs=[VM, HB, HB],
        out_specs=[VM] * 6,
        out_shape=[
            shape(BF16, 6, 2, 9, ROWS, 3 * C),
            shape(BF16, 6, 2, 7, ROWS, 3 * C),
            shape(BF16, 6, 2, 5, ROWS, 3 * C),
            shape(BF16, 36 * C, 2 * C),
            shape(BF16, 36 * C, 2 * C),
            shape(F32, 1, C),
        ],
        scratch_shapes=[pltpu.VMEM((FR, 3, 48, C), F32), pltpu.SemaphoreType.DMA((3,))],
        compiler_params=params(16),
        cost_estimate=pl.CostEstimate(flops=1_000_000_000, bytes_accessed=8_000_000, transcendentals=0),
        name="own_columns",
    )(own, w, bias)


def near(t, own, p, wp, wfp, bias, x3, g3, f3):
    return pl.pallas_call(
        near_kernel,
        in_specs=[SM] + [VM] * 8,
        out_specs=[VM] * 5,
        out_shape=[shape(v.dtype, *v.shape) for v in (x3, g3, f3)]
        + [shape(F32, FR, 7, ROWS, C), shape(F32, 8, C)],
        scratch_shapes=[
            pltpu.VMEM((FR, 3, 48, C), F32),
            pltpu.VMEM((FR, 9, ROWS, C), BF16),
            pltpu.VMEM((FR, 4, 48, C), F32),
            pltpu.VMEM((FR, 2, 48, C), F32),
        ],
        input_output_aliases={6: 0, 7: 1, 8: 2},
        compiler_params=params(24),
        cost_estimate=pl.CostEstimate(flops=4_000_000_000, bytes_accessed=8_000_000, transcendentals=0),
        name="near_columns",
    )(t, own, p, wp, wfp, bias, x3, g3, f3)


def far(t, own, b, wp, wfp, bias, sq, x3, g3, f3, bd):
    return pl.pallas_call(
        far_kernel,
        in_specs=[SM] + [VM] * 10,
        out_specs=[VM] * 6,
        out_shape=[shape(F32, 16, BLOCK, C)] * 2
        + [shape(v.dtype, *v.shape) for v in (x3, g3, f3, bd)],
        scratch_shapes=[
            pltpu.VMEM((FR, 3, 48, C), F32),
            pltpu.VMEM((FR, 9, ROWS, C), BF16),
            pltpu.VMEM((FR, 3, 48, C), F32),
            pltpu.VMEM((FR, 3, 48, C), F32),
            pltpu.VMEM((FR, 3, ROWS, C), F32),
            pltpu.VMEM((27 * C + 8, C), F32),
        ],
        input_output_aliases={7: 2, 8: 3, 9: 4, 10: 5},
        compiler_params=params(24),
        cost_estimate=pl.CostEstimate(flops=6_000_000_000, bytes_accessed=8_000_000, transcendentals=0),
        name="far_columns",
    )(t, own, b, wp, wfp, bias, sq, x3, g3, f3, bd)[:2]


def shards(clip_features, upstream, weight, conv_bias):
    w = weight.reshape(27 * C, C)
    bias = conv_bias.reshape(1, C)
    swap = [(i, i ^ 1) for i in range(TILES)]
    pairs = []
    for i in range(1, TILES - 1, 2):
        pairs += [(i, i + 1), (i + 1, i)]
    t = lax.axis_index("tile").astype(jnp.int32).reshape(1)
    in_hbm = lambda v: pltpu.with_memory_space_constraint(v, pltpu.HBM)
    own, edge = gather(t, in_hbm(clip_features), in_hbm(upstream))
    other = lax.ppermute(edge, "tile", pairs)
    partner = lax.ppermute(own, "tile", swap)
    x3, g3, f3, wp, wfp, bias = prepare(own, in_hbm(w), in_hbm(bias))
    x3, g3, f3, bd, sq = near(t, own, partner, wp, wfp, bias, x3, g3, f3)
    keep, send = far(t, own, other, wp, wfp, bias, sq, x3, g3, f3, bd)
    total = keep + lax.ppermute(send, "tile", swap)
    row = lax.broadcasted_iota(jnp.int32, (1, BLOCK, 1), 1)
    low = (row == 109) | (row == 111)
    rounded = lax.reduce_precision(total, 8, 7)
    total = jnp.where(low, total - rounded, total).astype(BF16)
    groups = [[2 * i + c for i in range(16)] for c in range(2)]
    got = lax.all_to_all(total, "tile", 0, 0, axis_index_groups=groups, tiled=True)
    mine = pl.pallas_call(
        middle_kernel,
        in_specs=[VM],
        out_specs=VM,
        out_shape=jax.ShapeDtypeStruct((8, BLOCK, C), BF16),
        compiler_params=params(4),
        name="middle_sum",
    )(got)
    everyone = lax.all_to_all(mine, "clip", 0, 0, tiled=True)
    grad, grad_bias, penalty = pl.pallas_call(
        last_kernel,
        in_specs=[VM],
        out_specs=[VM] * 3,
        out_shape=[
            jax.ShapeDtypeStruct((108, C), F32),
            jax.ShapeDtypeStruct((1, C), F32),
            jax.ShapeDtypeStruct((1, 1), F32),
        ],
        compiler_params=params(4),
        name="last_sum",
    )(everyone)
    return grad, grad_bias.reshape(C), penalty.reshape(())


def solution(mesh):
    in_specs = (P("clip", None, "tile", None, None), P("clip", None, "tile", None, None), P(), P())
    out_specs = (P("tile", None), P(), P())
    return jax.shard_map(shards, mesh=mesh, in_specs=in_specs, out_specs=out_specs, check_vma=False)
```
